32 devices in a mesh: parts: 2 (over x), snp: 16 (over z, y, core).
Axes of the slice: x: 2, y: 2, z: 4, core: 2. Of those that a mesh axis runs over, the one named last changes fastest.
Arguments:
- local_block: float32 [32768, 1024], P(('parts', 'snp')), parts along dimension 0, may hold values from -1 to 1, as said below
- next_block: float32 [32768, 1024], P(('parts', 'snp')), parts along dimension 0, may hold values from -1 to 1, as said below
- shrinkage: float32 [64, 1], replicated, may hold values from 0.3 to 1
- marginal: float32 [64, 32768], P(None, ('parts', 'snp')), parts along dimension 1, may hold values from -12 to 12
- warm_start: float32 [64, 32768], P(None, ('parts', 'snp')), parts along dimension 1, may hold values from -3 to 3
Outputs:
- solution: float32 [64, 32768], P(None, ('parts', 'snp')), parts along dimension 1
- residual: float32 [64, 32768], P(None, ('parts', 'snp')), parts along dimension 1
The draws below stay inside these ranges and needn't reach their ends.
There are 2 independent parts, one for each index of `parts`. The reference program is written for one: setup_inputs(seed, part) draws one part's arguments, and reference() takes and returns one part's arrays. A program takes and returns all parts, laid end to end along the dimension named above; an argument that names none is the same for every part. Nothing has to cross between parts.
Inputs may be any that keep to these rules, and one draw needn't show every extreme that they name: `local_block`: each 1024 x 1024 block of rows is symmetric with ones on its diagonal. `next_block`: inside each 1024 x 1024 block of rows, entries whose column index exceeds the row index are zero; the last block of rows is zero.
All inputs are finite; a program needn't handle non-finite values.
Results may differ from the reference program's by a relative error of at most 0.0003.
Values sent between devices are 32-bit elements; how exact they have to be, the bound alone decides.
A program may use at most 64 MiB of HBM per device.

```python
import math
import jax
import jax.numpy as jnp
from jax import lax

BLOCK = 1024
TRAITS = 64
ITERS = 3
NSNP = 16384


def draw_local_block(key, part):
    count = NSNP // BLOCK
    half = 0.5 / math.sqrt(2.0 * BLOCK)
    raw = jax.random.uniform(jax.random.fold_in(key, 11), (count, BLOCK, BLOCK), jnp.float32, -half, half)
    sym = (raw + jnp.swapaxes(raw, 1, 2)) * (1.0 / math.sqrt(2.0))
    unit = jnp.eye(BLOCK, dtype=jnp.float32)[None]
    blocks = sym * (1.0 - unit) + unit
    return blocks.reshape(NSNP, BLOCK)


def draw_next_block(key, part):
    count = NSNP // BLOCK
    half = 0.5 / math.sqrt(2.0 * BLOCK)
    raw = jax.random.uniform(jax.random.fold_in(key, 12), (count, BLOCK, BLOCK), jnp.float32, -half, half)
    rows = jnp.arange(BLOCK)[:, None]
    cols = jnp.arange(BLOCK)[None, :]
    lower = (cols <= rows).astype(jnp.float32)[None]
    keep = (jnp.arange(count) < count - 1).astype(jnp.float32)[:, None, None]
    return (raw * lower * keep).reshape(NSNP, BLOCK)


def draw_marginal(key, part):
    noise = jnp.clip(jax.random.normal(jax.random.fold_in(key, 13), (TRAITS, NSNP), jnp.float32), -4.0, 4.0)
    return noise


def block_scale(own_key, shape, split, smallest, top_value):
    loudness, own = 1.0, jax.random.fold_in(own_key, 6)
    for dim, shards_of in split:
        heights = jnp.exp(jax.random.uniform(jax.random.fold_in(own, dim), (shards_of,), jnp.float32, smallest / len(split), top_value / len(split)))
        loudness = loudness * jnp.repeat(heights, shape[dim] // shards_of).reshape([-1 if axis == dim else 1 for axis in range(len(shape))])
    return loudness


def bell_draw(rng, extent, scale, bound, shards=(), kind=jnp.bfloat16):
    array = scale * jax.random.normal(rng, extent, jnp.float32)
    if shards:
        array = array * block_scale(rng, extent, shards, -0.22, 0.18)
    return jnp.clip(array, -bound, bound).astype(kind)


def setup_inputs(seed: int = 0, part: int = 0) -> dict:
    seeds = jax.random.split(jax.random.key(seed), 6)
    part_splits = jax.random.split(jax.random.fold_in(seeds[5], part), 6)
    return {
        "local_block": draw_local_block(jax.random.fold_in(jax.random.fold_in(seeds[5], part), 71), part),
        "next_block": draw_next_block(jax.random.fold_in(jax.random.fold_in(seeds[5], part), 71), part),
        "shrinkage": jnp.clip(jnp.exp(jax.random.uniform(seeds[2], (TRAITS, 1), jnp.float32, math.log(0.3), math.log(1.0))), 0.3, 1.0),
        "marginal": draw_marginal(jax.random.fold_in(jax.random.fold_in(seeds[5], part), 71), part),
        "warm_start": bell_draw(part_splits[4], (TRAITS, NSNP), 0.5, 3.0, ((1, 16),), jnp.float32),
    }


HIGH = lax.Precision.HIGHEST


def operate(field, local_block, next_block, shrinkage):
    traits = field.shape[0]
    count = field.shape[1] // BLOCK
    blocks = field.reshape(traits, count, BLOCK)
    own_blocks = local_block.reshape(count, BLOCK, BLOCK)
    next_blocks = next_block.reshape(count, BLOCK, BLOCK)
    filler = jnp.zeros((traits, 1, BLOCK), field.dtype)
    own = jnp.einsum('tnb,nba->tna', blocks, own_blocks, precision=HIGH)
    upper = jnp.concatenate([blocks[:, 1:], filler], axis=1)
    forward = jnp.einsum('tnb,nab->tna', upper, next_blocks, precision=HIGH)
    backward = jnp.einsum('tnb,nba->tna', blocks, next_blocks, precision=HIGH)
    backward = jnp.concatenate([filler, backward[:, :-1]], axis=1)
    return (own + forward + backward).reshape(traits, count * BLOCK) + shrinkage * field


def reference(local_block, next_block, shrinkage, marginal, warm_start):
    solution = warm_start
    residual = marginal - operate(warm_start, local_block, next_block, shrinkage)
    direction = residual
    norm_now = jnp.sum(residual * residual, axis=1, keepdims=True)
    for step in range(ITERS):
        image = operate(direction, local_block, next_block, shrinkage)
        alpha = norm_now / jnp.sum(direction * image, axis=1, keepdims=True)
        solution = solution + alpha * direction
        residual = residual - alpha * image
        norm_next = jnp.sum(residual * residual, axis=1, keepdims=True)
        direction = residual + (norm_next / norm_now) * direction
        norm_now = norm_next
    return solution, residual
```

```python
import functools
import jax
import jax.numpy as jnp
from jax import lax
from jax.experimental import pallas as pl
from jax.experimental.pallas import tpu as pltpu
from jax.sharding import PartitionSpec as P

ITERS = 3
GROUPS = 2
TILE = 256
F32 = jnp.float32
BF16 = jnp.bfloat16
ROWS = (((1,), (0,)), ((), ()))
ACROSS = (((1,), (1,)), ((), ()))


def halves(value):
    high = value.astype(BF16)
    return high, (value - high.astype(F32)).astype(BF16)


def scalars(moment, ridge):
    def weigh(left, right, at):
        total = 0.0
        for i, a in enumerate(left):
            for j, b in enumerate(right):
                total = total + a * b * at(i + j)
        return total

    image_moment = lambda i: ridge * moment[i] + moment[i + 1]
    residual = [jnp.ones_like(ridge)]
    direction = residual
    update = [jnp.zeros_like(ridge)] * ITERS
    norm_now = moment[0]
    for step in range(ITERS):
        alpha = norm_now / weigh(direction, direction, image_moment)
        for i, e in enumerate(direction):
            update[i] = update[i] + alpha * e
        along = [ridge * e for e in direction] + [0.0]
        for i, e in enumerate(direction):
            along[i + 1] = along[i + 1] + e
        residual = residual + [0.0]
        residual = [c - alpha * a for c, a in zip(residual, along)]
        if step + 1 < ITERS:
            norm_next = weigh(residual, residual, lambda i: moment[i])
            ratio = norm_next / norm_now
            direction = [c + ratio * e for c, e in zip(residual, direction + [0.0])]
            norm_now = norm_next
    return update, residual


def kernel(
    n, slots, local_hbm, next_hbm, shrink_ref, marginal_ref, warm_ref, x_ref, r_ref,
    stage, lhi, llo, nhi, nlo, basis, total, vcat, upcat, upper, psend, precv,
    square, mine, others,
    load_sem, vs_sem, vr_sem, ps_sem, pr_sem, ms_sem, mr_sem,
):
    me = lax.axis_index("snp")
    traits, block = warm_ref.shape
    count = traits // GROUPS
    tiles = block // TILE
    barrier = pltpu.get_barrier_semaphore()
    for k in range(1, n):
        pl.semaphore_signal(barrier, inc=1, device_id={"snp": lax.rem(me + k, n)})

    def load(i):
        source, width = (next_hbm, (i + 1) * TILE) if i < tiles else (local_hbm, block)
        rows = pl.ds((i % tiles) * TILE, TILE)
        cols = pl.ds(0, width)
        slot = i % slots
        return pltpu.make_async_copy(
            source.at[rows, cols], stage.at[slot, :, cols], load_sem.at[slot]
        )

    for i in range(slots):
        load(i).start()

    def convert(i):
        load(i).wait()
        row = (i % tiles) * TILE
        width = (i + 1) * TILE if i < tiles else block
        for c in range(0, width, TILE):
            piece = stage[i % slots, :, c : c + TILE]
            if i >= tiles and c == row:
                a = lax.broadcasted_iota(jnp.int32, (TILE, TILE), 0)
                b = lax.broadcasted_iota(jnp.int32, (TILE, TILE), 1)
                piece = jnp.where(a == b, 0.0, piece)
            high, low = halves(piece)
            to_high, to_low = (nhi, nlo) if i < tiles else (lhi, llo)
            to_high[row : row + TILE, c : c + TILE] = high
            to_low[row : row + TILE, c : c + TILE] = low
        if i + slots < 2 * tiles:
            load(i + slots).start()

    def group(g):
        return pl.ds(g * count, count)

    def send_field(j, g):
        source = warm_ref.at[group(g)] if j == 0 else basis.at[j - 1, group(g)]
        return pltpu.make_async_remote_copy(
            src_ref=source, dst_ref=upper.at[j, group(g)],
            send_sem=vs_sem.at[j, g], recv_sem=vr_sem.at[j, g],
            device_id={"snp": jnp.maximum(me - 1, 0)},
        )

    def send_coupling(j, g):
        return pltpu.make_async_remote_copy(
            src_ref=psend.at[j, group(g)], dst_ref=precv.at[j, group(g)],
            send_sem=ps_sem.at[j, g], recv_sem=pr_sem.at[j, g],
            device_id={"snp": jnp.minimum(me + 1, n - 1)},
        )

    def times(left, g, high, low, dims, lo_k, hi_k):
        both = lax.dot_general(left[g, :, lo_k:hi_k], high, dims, preferred_element_type=F32)
        rest = lax.dot_general(left[g, :count, lo_k:hi_k], low, dims, preferred_element_type=F32)
        return both[:count] + both[count:] + rest

    def split_into(dest, g, value):
        high, low = halves(value)
        dest[g, :count] = high
        dest[g, count:] = low

    def field(j, g):
        return warm_ref[g * count : (g + 1) * count] if j == 0 else basis[j - 1, g * count : (g + 1) * count]

    def start_field(j, g):
        @pl.when(me > 0)
        def _():
            send_field(j, g).start()

    def coupling(j, g):
        split_into(vcat, g, field(j, g))
        for c in range(0, block, TILE):
            psend[j, g * count : (g + 1) * count, c : c + TILE] = times(
                vcat, g, nhi[c:, c : c + TILE], nlo[c:, c : c + TILE], ROWS, c, block
            )

        @pl.when(me < n - 1)
        def _():
            send_coupling(j, g).start()

    def own(j, g):
        for c in range(0, block, TILE):
            total[g, :, c : c + TILE] = times(
                vcat, g, lhi[:, c : c + TILE], llo[:, c : c + TILE], ROWS, 0, block
            )

    def finish(j, g):
        rows = slice(g * count, (g + 1) * count)

        @pl.when(me < n - 1)
        def _():
            send_field(j, g).wait_recv()

        split_into(upcat, g, upper[j, rows])
        for c in range(0, block, TILE):
            end = c + TILE
            total[g, :, c:end] += times(upcat, g, nhi[c:end, :end], nlo[c:end, :end], ACROSS, 0, end)

        @pl.when(me > 0)
        def _():
            send_coupling(j, g).wait_recv()

        image = total[g] + precv[j, rows]
        if j == 0:
            image = marginal_ref[rows] - (1.0 + shrink_ref[rows]) * warm_ref[rows] - image
        basis[j, rows] = image

    @pl.when(me == 0)
    def _():
        precv[...] = jnp.zeros_like(precv)

    @pl.when(me == n - 1)
    def _():
        upper[...] = jnp.zeros_like(upper)

    pl.semaphore_wait(barrier, n - 1)
    for g in range(GROUPS):
        start_field(0, g)
    for i in range(tiles):
        convert(i)
    for g in range(GROUPS):
        coupling(0, g)
    for i in range(tiles, 2 * tiles):
        convert(i)
    for g in range(GROUPS):
        own(0, g)
    for j in range(ITERS + 1):
        for g in range(GROUPS):
            finish(j, g)
            if j < ITERS:
                start_field(j + 1, g)
                coupling(j + 1, g)
                own(j + 1, g)

    lane = lax.broadcasted_iota(jnp.int32, (traits, 128), 1)
    table = jnp.where(lane == 6, 1.0 + shrink_ref[...], 0.0)
    for k in range(2 * ITERS):
        sums = jnp.sum(basis[k // 2] * basis[(k + 1) // 2], axis=1, keepdims=True)
        table = jnp.where(lane == k, sums, table)
    square[...] = jnp.zeros_like(square)
    square[:traits] = table
    flat = jnp.transpose(square[...])
    mine[...] = flat[:8]
    others[me] = flat[:8]

    def send_sums(k):
        return pltpu.make_async_remote_copy(
            src_ref=mine, dst_ref=others.at[me],
            send_sem=ms_sem.at[k], recv_sem=mr_sem.at[me],
            device_id={"snp": lax.rem(me + k, n)},
        )

    def take_sums(k):
        source = lax.rem(me + k, n)
        return pltpu.make_async_remote_copy(
            src_ref=mine, dst_ref=others.at[source],
            send_sem=ms_sem.at[k], recv_sem=mr_sem.at[source],
            device_id={"snp": source},
        )

    for k in range(1, n):
        send_sums(k).start()
    for k in range(1, n):
        take_sums(k).wait_recv()
    sums = others[0]
    for k in range(1, n):
        sums = sums + others[k]
    moment = [sums[k : k + 1] for k in range(2 * ITERS)]
    update, residual = scalars(moment, mine[6:7])
    for k, row in enumerate(update + residual):
        square[k : k + 1] = row
    tall = jnp.transpose(square[...])[:traits]
    x = warm_ref[...]
    for k in range(ITERS):
        x = x + tall[:, k : k + 1] * basis[k]
    x_ref[...] = x
    r = tall[:, ITERS : ITERS + 1] * basis[0]
    for k in range(1, ITERS + 1):
        r = r + tall[:, ITERS + k : ITERS + k + 1] * basis[k]
    r_ref[...] = r

    for k in range(1, n):
        send_sums(k).wait_send()

    @pl.when(me > 0)
    def _():
        for j in range(ITERS + 1):
            for g in range(GROUPS):
                send_field(j, g).wait_send()

    @pl.when(me < n - 1)
    def _():
        for j in range(ITERS + 1):
            for g in range(GROUPS):
                send_coupling(j, g).wait_send()


def on_device(local_block, next_block, shrinkage, marginal, warm_start):
    n = lax.axis_size("snp")
    traits, block = warm_start.shape
    count = traits // GROUPS
    slots = min(2 * (block // TILE), 8 if block <= 1024 else 4)
    apps = ITERS + 1
    vmem = pl.BlockSpec(memory_space=pltpu.VMEM)
    field = (apps, traits, block)
    return pl.pallas_call(
        functools.partial(kernel, n, slots),
        name="cg",
        out_shape=[jax.ShapeDtypeStruct((traits, block), F32)] * 2,
        in_specs=[pl.BlockSpec(memory_space=pltpu.HBM)] * 2 + [vmem] * 3,
        out_specs=[vmem] * 2,
        scratch_shapes=[
            pltpu.VMEM((slots, TILE, block), F32),
            pltpu.VMEM((block, block), BF16),
            pltpu.VMEM((block, block), BF16),
            pltpu.VMEM((block, block), BF16),
            pltpu.VMEM((block, block), BF16),
            pltpu.VMEM(field, F32),
            pltpu.VMEM((GROUPS, count, block), F32),
            pltpu.VMEM((GROUPS, 2 * count, block), BF16),
            pltpu.VMEM((GROUPS, 2 * count, block), BF16),
            pltpu.VMEM(field, F32),
            pltpu.VMEM(field, F32),
            pltpu.VMEM(field, F32),
            pltpu.VMEM((128, 128), F32),
            pltpu.VMEM((8, 128), F32),
            pltpu.VMEM((n, 8, 128), F32),
            pltpu.SemaphoreType.DMA((slots,)),
            pltpu.SemaphoreType.DMA((apps, GROUPS)),
            pltpu.SemaphoreType.DMA((apps, GROUPS)),
            pltpu.SemaphoreType.DMA((apps, GROUPS)),
            pltpu.SemaphoreType.DMA((apps, GROUPS)),
            pltpu.SemaphoreType.DMA((n,)),
            pltpu.SemaphoreType.DMA((n,)),
        ],
        compiler_params=pltpu.CompilerParams(
            collective_id=0, has_side_effects=True, vmem_limit_bytes=67043328
        ),
    )(local_block, next_block, shrinkage, marginal, warm_start)


def solution(mesh):
    return jax.shard_map(
        on_device,
        mesh=mesh,
        in_specs=(
            P(("parts", "snp"), None),
            P(("parts", "snp"), None),
            P(),
            P(None, ("parts", "snp")),
            P(None, ("parts", "snp")),
        ),
        out_specs=(P(None, ("parts", "snp")), P(None, ("parts", "snp"))),
        check_vma=False,
    )
```

```python
import functools
import jax
import jax.numpy as jnp
from jax import lax
from jax.experimental import pallas as pl
from jax.experimental.pallas import tpu as pltpu
from jax.sharding import PartitionSpec as P

ITERS = 3
GROUPS = 2
TILE = 256
F32 = jnp.float32
BF16 = jnp.bfloat16
ROWS = (((1,), (0,)), ((), ()))
ACROSS = (((1,), (1,)), ((), ()))


def halves(value):
    high = value.astype(BF16)
    return high, (value - high.astype(F32)).astype(BF16)


def scalars(moment, ridge):
    def weigh(left, right, at):
        total = 0.0
        for i, a in enumerate(left):
            for j, b in enumerate(right):
                total = total + a * b * at(i + j)
        return total

    image_moment = lambda i: ridge * moment[i] + moment[i + 1]
    residual = [jnp.ones_like(ridge)]
    direction = residual
    update = [jnp.zeros_like(ridge)] * ITERS
    norm_now = moment[0]
    for step in range(ITERS):
        alpha = norm_now / weigh(direction, direction, image_moment)
        for i, e in enumerate(direction):
            update[i] = update[i] + alpha * e
        along = [ridge * e for e in direction] + [0.0]
        for i, e in enumerate(direction):
            along[i + 1] = along[i + 1] + e
        residual = residual + [0.0]
        residual = [c - alpha * a for c, a in zip(residual, along)]
        if step + 1 < ITERS:
            norm_next = weigh(residual, residual, lambda i: moment[i])
            ratio = norm_next / norm_now
            direction = [c + ratio * e for c, e in zip(residual, direction + [0.0])]
            norm_now = norm_next
    return update, residual


def kernel(
    n, slots, local_hbm, next_hbm, shrink_ref, marginal_ref, warm_ref, x_ref, r_ref,
    stage, lhi, llo, nhi, nlo, basis, total, vcat, upcat, upper, psend, precv,
    square, table, ridge, mine, others,
    load_sem, vs_sem, vr_sem, ps_sem, pr_sem, ms_sem, mr_sem,
):
    me = lax.axis_index("snp")
    traits, block = warm_ref.shape
    count = traits // GROUPS
    tiles = block // TILE
    barrier = pltpu.get_barrier_semaphore()
    for k in range(1, n):
        pl.semaphore_signal(barrier, inc=1, device_id={"snp": lax.rem(me + k, n)})

    lane = lax.broadcasted_iota(jnp.int32, (count, 128), 1)
    square[...] = jnp.zeros_like(square)
    square[0:1, :traits] = 1.0 + shrink_ref[...]
    ridge[...] = jnp.transpose(square[...])[:traits]

    def load(i):
        source, width = (next_hbm, (i + 1) * TILE) if i < tiles else (local_hbm, block)
        rows = pl.ds((i % tiles) * TILE, TILE)
        cols = pl.ds(0, width)
        slot = i % slots
        return pltpu.make_async_copy(
            source.at[rows, cols], stage.at[slot, :, cols], load_sem.at[slot]
        )

    for i in range(slots):
        load(i).start()

    def convert(i):
        load(i).wait()
        row = (i % tiles) * TILE
        width = (i + 1) * TILE if i < tiles else block
        for c in range(0, width, TILE):
            piece = stage[i % slots, :, c : c + TILE]
            if i >= tiles and c == row:
                a = lax.broadcasted_iota(jnp.int32, (TILE, TILE), 0)
                b = lax.broadcasted_iota(jnp.int32, (TILE, TILE), 1)
                piece = jnp.where(a == b, 0.0, piece)
            high, low = halves(piece)
            to_high, to_low = (nhi, nlo) if i < tiles else (lhi, llo)
            to_high[row : row + TILE, c : c + TILE] = high
            to_low[row : row + TILE, c : c + TILE] = low
        if i + slots < 2 * tiles:
            load(i + slots).start()

    def group(g):
        return pl.ds(g * count, count)

    def send_field(j, g):
        source = warm_ref.at[group(g)] if j == 0 else basis.at[j - 1, group(g)]
        return pltpu.make_async_remote_copy(
            src_ref=source, dst_ref=upper.at[j, group(g)],
            send_sem=vs_sem.at[j, g], recv_sem=vr_sem.at[j, g],
            device_id={"snp": jnp.maximum(me - 1, 0)},
        )

    def send_coupling(j, g):
        return pltpu.make_async_remote_copy(
            src_ref=psend.at[j, group(g)], dst_ref=precv.at[j, group(g)],
            send_sem=ps_sem.at[j, g], recv_sem=pr_sem.at[j, g],
            device_id={"snp": jnp.minimum(me + 1, n - 1)},
        )

    def times(left, g, high, low, dims, lo_k, hi_k):
        both = lax.dot_general(left[g, :, lo_k:hi_k], high, dims, preferred_element_type=F32)
        rest = lax.dot_general(left[g, :count, lo_k:hi_k], low, dims, preferred_element_type=F32)
        return both[:count] + both[count:] + rest

    def split_into(dest, g, value):
        high, low = halves(value)
        dest[g, :count] = high
        dest[g, count:] = low

    def field(j, g):
        return warm_ref[g * count : (g + 1) * count] if j == 0 else basis[j - 1, g * count : (g + 1) * count]

    def start_field(j, g):
        @pl.when(me > 0)
        def _():
            send_field(j, g).start()

    def coupling(j, g):
        split_into(vcat, g, field(j, g))
        for c in range(0, block, TILE):
            psend[j, g * count : (g + 1) * count, c : c + TILE] = times(
                vcat, g, nhi[c:, c : c + TILE], nlo[c:, c : c + TILE], ROWS, c, block
            )

        @pl.when(me < n - 1)
        def _():
            send_coupling(j, g).start()

    def own(j, g):
        for c in range(0, block, TILE):
            total[g, :, c : c + TILE] = times(
                vcat, g, lhi[:, c : c + TILE], llo[:, c : c + TILE], ROWS, 0, block
            )

    def meet(j, g):
        rows = slice(g * count, (g + 1) * count)

        @pl.when(me < n - 1)
        def _():
            send_field(j, g).wait_recv()

        split_into(upcat, g, upper[j, rows])
        last = jnp.zeros((count, TILE), F32)
        for c in range(0, block, TILE):
            end = c + TILE
            forward = times(upcat, g, nhi[c:end, :end], nlo[c:end, :end], ACROSS, 0, end)
            image = total[g, :, c:end] + forward
            if j == ITERS:
                last += basis[j - 1, rows, c:end] * (image + forward)
            total[g, :, c:end] = image
        if j == ITERS:
            last = jnp.sum(last, axis=1, keepdims=True)
            table[rows] = jnp.where(lane == 2 * ITERS - 1, last, table[rows])

    def finish(j, g):
        rows = slice(g * count, (g + 1) * count)

        @pl.when(me > 0)
        def _():
            send_coupling(j, g).wait_recv()

        image = total[g] + precv[j, rows]
        if j == 0:
            image = marginal_ref[rows] - ridge[rows, :1] * warm_ref[rows] - image
        basis[j, rows] = image

    def moments(g):
        rows = slice(g * count, (g + 1) * count)
        kept = jnp.where(lane == 2 * ITERS, ridge[rows, :1], 0.0)
        for k in range(2 * ITERS - 1):
            sums = jnp.sum(basis[k // 2, rows] * basis[(k + 1) // 2, rows], axis=1, keepdims=True)
            kept = jnp.where(lane == k, sums, kept)
        table[rows] = kept

    @pl.when(me == 0)
    def _():
        precv[...] = jnp.zeros_like(precv)

    @pl.when(me == n - 1)
    def _():
        upper[...] = jnp.zeros_like(upper)

    pl.semaphore_wait(barrier, n - 1)
    for g in range(GROUPS):
        start_field(0, g)
    for i in range(tiles):
        convert(i)
    for g in range(GROUPS):
        coupling(0, g)
    for i in range(tiles, 2 * tiles):
        convert(i)
    for g in range(GROUPS):
        own(0, g)
    for j in range(ITERS):
        for g in range(GROUPS):
            meet(j, g)
            finish(j, g)
            start_field(j + 1, g)
            coupling(j + 1, g)
            own(j + 1, g)
            if j + 1 == ITERS:
                moments(g)
    for g in range(GROUPS):
        meet(ITERS, g)

    square[:traits] = table[...]
    flat = jnp.transpose(square[...])
    mine[...] = flat[:8]
    others[me] = flat[:8]

    def send_sums(k):
        return pltpu.make_async_remote_copy(
            src_ref=mine, dst_ref=others.at[me],
            send_sem=ms_sem.at[k], recv_sem=mr_sem.at[me],
            device_id={"snp": lax.rem(me + k, n)},
        )

    def take_sums(k):
        source = lax.rem(me + k, n)
        return pltpu.make_async_remote_copy(
            src_ref=mine, dst_ref=others.at[source],
            send_sem=ms_sem.at[k], recv_sem=mr_sem.at[source],
            device_id={"snp": source},
        )

    for k in range(1, n):
        send_sums(k).start()
    for g in range(GROUPS):
        finish(ITERS, g)
    for k in range(1, n):
        take_sums(k).wait_recv()
    sums = others[0]
    for k in range(1, n):
        sums = sums + others[k]
    moment = [sums[k : k + 1] for k in range(2 * ITERS)]
    update, residual = scalars(moment, mine[2 * ITERS : 2 * ITERS + 1])
    for k, row in enumerate(update + residual):
        square[k : k + 1] = row
    tall = jnp.transpose(square[...])[:traits]
    x = warm_ref[...]
    for k in range(ITERS):
        x = x + tall[:, k : k + 1] * basis[k]
    x_ref[...] = x
    r = tall[:, ITERS : ITERS + 1] * basis[0]
    for k in range(1, ITERS + 1):
        r = r + tall[:, ITERS + k : ITERS + k + 1] * basis[k]
    r_ref[...] = r

    for k in range(1, n):
        send_sums(k).wait_send()

    @pl.when(me > 0)
    def _():
        for j in range(ITERS + 1):
            for g in range(GROUPS):
                send_field(j, g).wait_send()

    @pl.when(me < n - 1)
    def _():
        for j in range(ITERS + 1):
            for g in range(GROUPS):
                send_coupling(j, g).wait_send()


def on_device(local_block, next_block, shrinkage, marginal, warm_start):
    n = lax.axis_size("snp")
    traits, block = warm_start.shape
    count = traits // GROUPS
    slots = min(2 * (block // TILE), 8 if block <= 1024 else 4)
    apps = ITERS + 1
    vmem = pl.BlockSpec(memory_space=pltpu.VMEM)
    field = (apps, traits, block)
    return pl.pallas_call(
        functools.partial(kernel, n, slots),
        name="cg",
        out_shape=[jax.ShapeDtypeStruct((traits, block), F32)] * 2,
        in_specs=[pl.BlockSpec(memory_space=pltpu.HBM)] * 2 + [vmem] * 3,
        out_specs=[vmem] * 2,
        scratch_shapes=[
            pltpu.VMEM((slots, TILE, block), F32),
            pltpu.VMEM((block, block), BF16),
            pltpu.VMEM((block, block), BF16),
            pltpu.VMEM((block, block), BF16),
            pltpu.VMEM((block, block), BF16),
            pltpu.VMEM(field, F32),
            pltpu.VMEM((GROUPS, count, block), F32),
            pltpu.VMEM((GROUPS, 2 * count, block), BF16),
            pltpu.VMEM((GROUPS, 2 * count, block), BF16),
            pltpu.VMEM(field, F32),
            pltpu.VMEM(field, F32),
            pltpu.VMEM(field, F32),
            pltpu.VMEM((128, 128), F32),
            pltpu.VMEM((traits, 128), F32),
            pltpu.VMEM((traits, 128), F32),
            pltpu.VMEM((8, 128), F32),
            pltpu.VMEM((n, 8, 128), F32),
            pltpu.SemaphoreType.DMA((slots,)),
            pltpu.SemaphoreType.DMA((apps, GROUPS)),
            pltpu.SemaphoreType.DMA((apps, GROUPS)),
            pltpu.SemaphoreType.DMA((apps, GROUPS)),
            pltpu.SemaphoreType.DMA((apps, GROUPS)),
            pltpu.SemaphoreType.DMA((n,)),
            pltpu.SemaphoreType.DMA((n,)),
        ],
        compiler_params=pltpu.CompilerParams(
            collective_id=0, has_side_effects=True, vmem_limit_bytes=61 << 20
        ),
    )(local_block, next_block, shrinkage.reshape(1, traits), marginal, warm_start)


def solution(mesh):
    return jax.shard_map(
        on_device,
        mesh=mesh,
        in_specs=(
            P(("parts", "snp"), None),
            P(("parts", "snp"), None),
            P(),
            P(None, ("parts", "snp")),
            P(None, ("parts", "snp")),
        ),
        out_specs=(P(None, ("parts", "snp")), P(None, ("parts", "snp"))),
        check_vma=False,
    )
```

```python
import functools
import jax
import jax.numpy as jnp
from jax import lax
from jax.experimental import pallas as pl
from jax.experimental.pallas import tpu as pltpu
from jax.sharding import PartitionSpec as P

ITERS = 3
GROUPS = 2
TILE = 256
F32 = jnp.float32
BF16 = jnp.bfloat16
ROWS = (((1,), (0,)), ((), ()))
ACROSS = (((1,), (1,)), ((), ()))


def halves(value):
    high = value.astype(BF16)
    return high, (value - high.astype(F32)).astype(BF16)


def scalars(moment, ridge):
    def weigh(left, right, at):
        total = 0.0
        for i, a in enumerate(left):
            for j, b in enumerate(right):
                total = total + a * b * at(i + j)
        return total

    image_moment = lambda i: ridge * moment[i] + moment[i + 1]
    residual = [jnp.ones_like(ridge)]
    direction = residual
    update = [jnp.zeros_like(ridge)] * ITERS
    norm_now = moment[0]
    for step in range(ITERS):
        alpha = norm_now / weigh(direction, direction, image_moment)
        for i, e in enumerate(direction):
            update[i] = update[i] + alpha * e
        along = [ridge * e for e in direction] + [0.0]
        for i, e in enumerate(direction):
            along[i + 1] = along[i + 1] + e
        residual = residual + [0.0]
        residual = [c - alpha * a for c, a in zip(residual, along)]
        if step + 1 < ITERS:
            norm_next = weigh(residual, residual, lambda i: moment[i])
            ratio = norm_next / norm_now
            direction = [c + ratio * e for c, e in zip(residual, direction + [0.0])]
            norm_now = norm_next
    return update, residual


def kernel(
    n, slots, local_hbm, next_hbm, shrink_ref, marginal_hbm, warm_hbm, x_ref, r_ref,
    marginal_ref, warm_ref, stage, lhi, llo, nhi, nlo, basis, total, vcat, upcat, upper, psend, precv,
    square, table, ridge, mine, others,
    field_sem, load_sem, vs_sem, vr_sem, ps_sem, pr_sem, ms_sem, mr_sem,
):
    me = lax.axis_index("snp")
    traits, block = warm_ref.shape
    count = traits // GROUPS
    tiles = block // TILE
    warm_load = pltpu.make_async_copy(warm_hbm, warm_ref, field_sem.at[0])
    warm_load.start()
    barrier = pltpu.get_barrier_semaphore()
    for k in range(1, n):
        pl.semaphore_signal(barrier, inc=1, device_id={"snp": lax.rem(me + k, n)})

    lane = lax.broadcasted_iota(jnp.int32, (count, 128), 1)
    square[...] = jnp.zeros_like(square)
    square[0:1, :traits] = 1.0 + shrink_ref[...]
    ridge[...] = jnp.transpose(square[...])[:traits]

    def load(i):
        source, width = (next_hbm, (i + 1) * TILE) if i < tiles else (local_hbm, block)
        rows = pl.ds((i % tiles) * TILE, TILE)
        cols = pl.ds(0, width)
        slot = i % slots
        return pltpu.make_async_copy(
            source.at[rows, cols], stage.at[slot, :, cols], load_sem.at[slot]
        )

    for i in range(slots):
        load(i).start()
    marginal_load = pltpu.make_async_copy(marginal_hbm, marginal_ref, field_sem.at[1])
    marginal_load.start()

    def convert(i):
        load(i).wait()
        row = (i % tiles) * TILE
        width = (i + 1) * TILE if i < tiles else block
        for c in range(0, width, TILE):
            piece = stage[i % slots, :, c : c + TILE]
            if i >= tiles and c == row:
                a = lax.broadcasted_iota(jnp.int32, (TILE, TILE), 0)
                b = lax.broadcasted_iota(jnp.int32, (TILE, TILE), 1)
                piece = jnp.where(a == b, 0.0, piece)
            high, low = halves(piece)
            to_high, to_low = (nhi, nlo) if i < tiles else (lhi, llo)
            to_high[row : row + TILE, c : c + TILE] = high
            to_low[row : row + TILE, c : c + TILE] = low
        if i + slots < 2 * tiles:
            load(i + slots).start()

    def group(g):
        return pl.ds(g * count, count)

    def send_field(j, g):
        source = warm_ref.at[group(g)] if j == 0 else basis.at[j - 1, group(g)]
        return pltpu.make_async_remote_copy(
            src_ref=source, dst_ref=upper.at[j, group(g)],
            send_sem=vs_sem.at[j, g], recv_sem=vr_sem.at[j, g],
            device_id={"snp": jnp.maximum(me - 1, 0)},
        )

    def send_coupling(j, g):
        return pltpu.make_async_remote_copy(
            src_ref=psend.at[j, group(g)], dst_ref=precv.at[j, group(g)],
            send_sem=ps_sem.at[j, g], recv_sem=pr_sem.at[j, g],
            device_id={"snp": jnp.minimum(me + 1, n - 1)},
        )

    def times(left, g, high, low, dims, lo_k, hi_k):
        both = lax.dot_general(left[g, :, lo_k:hi_k], high, dims, preferred_element_type=F32)
        rest = lax.dot_general(left[g, :count, lo_k:hi_k], low, dims, preferred_element_type=F32)
        return both[:count] + both[count:] + rest

    def split_into(dest, g, value):
        high, low = halves(value)
        dest[g, :count] = high
        dest[g, count:] = low

    def field(j, g):
        return warm_ref[g * count : (g + 1) * count] if j == 0 else basis[j - 1, g * count : (g + 1) * count]

    def start_field(j, g):
        @pl.when(me > 0)
        def _():
            send_field(j, g).start()

    def coupling(j, g):
        split_into(vcat, g, field(j, g))
        for c in range(0, block, TILE):
            psend[j, g * count : (g + 1) * count, c : c + TILE] = times(
                vcat, g, nhi[c:, c : c + TILE], nlo[c:, c : c + TILE], ROWS, c, block
            )

        @pl.when(me < n - 1)
        def _():
            send_coupling(j, g).start()

    def own(j, g):
        for c in range(0, block, TILE):
            total[g, :, c : c + TILE] = times(
                vcat, g, lhi[:, c : c + TILE], llo[:, c : c + TILE], ROWS, 0, block
            )

    def meet(j, g):
        rows = slice(g * count, (g + 1) * count)

        @pl.when(me < n - 1)
        def _():
            send_field(j, g).wait_recv()

        split_into(upcat, g, upper[j, rows])
        last = jnp.zeros((count, TILE), F32)
        for c in range(0, block, TILE):
            end = c + TILE
            forward = times(upcat, g, nhi[c:end, :end], nlo[c:end, :end], ACROSS, 0, end)
            image = total[g, :, c:end] + forward
            if j == ITERS:
                last += basis[j - 1, rows, c:end] * (image + forward)
            total[g, :, c:end] = image
        if j == ITERS:
            last = jnp.sum(last, axis=1, keepdims=True)
            table[rows] = jnp.where(lane == 2 * ITERS - 1, last, table[rows])

    def finish(j, g):
        rows = slice(g * count, (g + 1) * count)

        @pl.when(me > 0)
        def _():
            send_coupling(j, g).wait_recv()

        image = total[g] + precv[j, rows]
        if j == 0:
            image = marginal_ref[rows] - ridge[rows, :1] * warm_ref[rows] - image
        basis[j, rows] = image

    def moments(g):
        rows = slice(g * count, (g + 1) * count)
        kept = jnp.where(lane == 2 * ITERS, ridge[rows, :1], 0.0)
        for k in range(2 * ITERS - 1):
            sums = jnp.sum(basis[k // 2, rows] * basis[(k + 1) // 2, rows], axis=1, keepdims=True)
            kept = jnp.where(lane == k, sums, kept)
        table[rows] = kept

    @pl.when(me == 0)
    def _():
        precv[...] = jnp.zeros_like(precv)

    @pl.when(me == n - 1)
    def _():
        upper[...] = jnp.zeros_like(upper)

    warm_load.wait()
    for i in range(tiles):
        convert(i)
    pl.semaphore_wait(barrier, n - 1)
    for g in range(GROUPS):
        start_field(0, g)
    for g in range(GROUPS):
        coupling(0, g)
    for i in range(tiles, 2 * tiles):
        convert(i)
    for g in range(GROUPS):
        own(0, g)
    marginal_load.wait()
    for j in range(ITERS):
        for g in range(GROUPS):
            meet(j, g)
            finish(j, g)
            start_field(j + 1, g)
            coupling(j + 1, g)
            own(j + 1, g)
            if j + 1 == ITERS:
                moments(g)
    for g in range(GROUPS):
        meet(ITERS, g)

    square[:traits] = table[...]
    flat = jnp.transpose(square[...])
    mine[...] = flat[:8]
    others[me] = flat[:8]

    def send_sums(k):
        return pltpu.make_async_remote_copy(
            src_ref=mine, dst_ref=others.at[me],
            send_sem=ms_sem.at[k], recv_sem=mr_sem.at[me],
            device_id={"snp": lax.rem(me + k, n)},
        )

    def take_sums(k):
        source = lax.rem(me + k, n)
        return pltpu.make_async_remote_copy(
            src_ref=mine, dst_ref=others.at[source],
            send_sem=ms_sem.at[k], recv_sem=mr_sem.at[source],
            device_id={"snp": source},
        )

    for k in range(1, n):
        send_sums(k).start()
    for k in range(1, n):
        take_sums(k).wait_recv()
    sums = others[0]
    for k in range(1, n):
        sums = sums + others[k]
    moment = [sums[k : k + 1] for k in range(2 * ITERS)]
    update, residual = scalars(moment, mine[2 * ITERS : 2 * ITERS + 1])
    for k, row in enumerate(update + residual):
        square[k : k + 1] = row
    tall = jnp.transpose(square[...])[:traits]
    x = warm_ref[...]
    for k in range(ITERS):
        x = x + tall[:, k : k + 1] * basis[k]
    x_ref[...] = x
    for g in range(GROUPS):
        rows = slice(g * count, (g + 1) * count)
        r = tall[rows, 2 * ITERS : 2 * ITERS + 1] * total[g]
        for k in range(ITERS):
            r = r + tall[rows, ITERS + k : ITERS + k + 1] * basis[k, rows]
        r_ref[rows] = r
    for g in range(GROUPS):
        rows = slice(g * count, (g + 1) * count)

        @pl.when(me > 0)
        def _():
            send_coupling(ITERS, g).wait_recv()

        r_ref[rows] += tall[rows, 2 * ITERS : 2 * ITERS + 1] * precv[ITERS, rows]

    for k in range(1, n):
        send_sums(k).wait_send()

    @pl.when(me > 0)
    def _():
        for j in range(ITERS + 1):
            for g in range(GROUPS):
                send_field(j, g).wait_send()

    @pl.when(me < n - 1)
    def _():
        for j in range(ITERS + 1):
            for g in range(GROUPS):
                send_coupling(j, g).wait_send()


def hand_on(x_in, r_in, x_ref, r_ref):
    x_ref[...] = x_in[...]
    r_ref[...] = r_in[...]


def on_device(local_block, next_block, shrinkage, marginal, warm_start):
    n = lax.axis_size("snp")
    traits, block = warm_start.shape
    count = traits // GROUPS
    slots = min(2 * (block // TILE), 8 if block <= 1024 else 4)
    apps = ITERS + 1
    vmem = pl.BlockSpec(memory_space=pltpu.VMEM)
    hbm = pl.BlockSpec(memory_space=pltpu.HBM)
    field = (apps, traits, block)
    x, r = pl.pallas_call(
        functools.partial(kernel, n, slots),
        name="cg",
        out_shape=[jax.ShapeDtypeStruct((traits, block), F32)] * 2,
        in_specs=[hbm, hbm, vmem, hbm, hbm],
        out_specs=[vmem] * 2,
        scratch_shapes=[
            pltpu.VMEM((traits, block), F32),
            pltpu.VMEM((traits, block), F32),
            pltpu.VMEM((slots, TILE, block), F32),
            pltpu.VMEM((block, block), BF16),
            pltpu.VMEM((block, block), BF16),
            pltpu.VMEM((block, block), BF16),
            pltpu.VMEM((block, block), BF16),
            pltpu.VMEM((ITERS, traits, block), F32),
            pltpu.VMEM((GROUPS, count, block), F32),
            pltpu.VMEM((GROUPS, 2 * count, block), BF16),
            pltpu.VMEM((GROUPS, 2 * count, block), BF16),
            pltpu.VMEM(field, F32),
            pltpu.VMEM(field, F32),
            pltpu.VMEM(field, F32),
            pltpu.VMEM((128, 128), F32),
            pltpu.VMEM((traits, 128), F32),
            pltpu.VMEM((traits, 128), F32),
            pltpu.VMEM((8, 128), F32),
            pltpu.VMEM((n, 8, 128), F32),
            pltpu.SemaphoreType.DMA((2,)),
            pltpu.SemaphoreType.DMA((slots,)),
            pltpu.SemaphoreType.DMA((apps, GROUPS)),
            pltpu.SemaphoreType.DMA((apps, GROUPS)),
            pltpu.SemaphoreType.DMA((apps, GROUPS)),
            pltpu.SemaphoreType.DMA((apps, GROUPS)),
            pltpu.SemaphoreType.DMA((n,)),
            pltpu.SemaphoreType.DMA((n,)),
        ],
        compiler_params=pltpu.CompilerParams(
            collective_id=0, has_side_effects=True, vmem_limit_bytes=61 << 20
        ),
    )(local_block, next_block, shrinkage.reshape(1, traits), marginal, warm_start)
    return pl.pallas_call(
        hand_on,
        name="hand_on",
        out_shape=[jax.ShapeDtypeStruct((traits, block), F32)] * 2,
        in_specs=[vmem] * 2,
        out_specs=[vmem] * 2,
    )(x, r)


def solution(mesh):
    return jax.shard_map(
        on_device,
        mesh=mesh,
        in_specs=(
            P(("parts", "snp"), None),
            P(("parts", "snp"), None),
            P(),
            P(None, ("parts", "snp")),
            P(None, ("parts", "snp")),
        ),
        out_specs=(P(None, ("parts", "snp")), P(None, ("parts", "snp"))),
        check_vma=False,
    )
```

```python
import functools
import jax
import jax.numpy as jnp
from jax import lax
from jax.experimental import pallas as pl
from jax.experimental.pallas import tpu as pltpu
from jax.sharding import PartitionSpec as P

ITERS = 3
GROUPS = 2
TILE = 256
F32 = jnp.float32
BF16 = jnp.bfloat16
ROWS = (((1,), (0,)), ((), ()))
ACROSS = (((1,), (1,)), ((), ()))


def halves(value):
    high = value.astype(BF16)
    return high, (value - high.astype(F32)).astype(BF16)


def scalars(moment, ridge):
    def weigh(left, right, at):
        total = 0.0
        for i, a in enumerate(left):
            for j, b in enumerate(right):
                total = total + a * b * at(i + j)
        return total

    image_moment = lambda i: ridge * moment[i] + moment[i + 1]
    residual = [jnp.ones_like(ridge)]
    direction = residual
    update = [jnp.zeros_like(ridge)] * ITERS
    norm_now = moment[0]
    for step in range(ITERS):
        alpha = norm_now / weigh(direction, direction, image_moment)
        for i, e in enumerate(direction):
            update[i] = update[i] + alpha * e
        along = [ridge * e for e in direction] + [0.0]
        for i, e in enumerate(direction):
            along[i + 1] = along[i + 1] + e
        residual = residual + [0.0]
        residual = [c - alpha * a for c, a in zip(residual, along)]
        if step + 1 < ITERS:
            norm_next = weigh(residual, residual, lambda i: moment[i])
            ratio = norm_next / norm_now
            direction = [c + ratio * e for c, e in zip(residual, direction + [0.0])]
            norm_now = norm_next
    return update, residual


def kernel(
    n, slots, local_hbm, next_hbm, shrink_ref, marginal_hbm, warm_hbm, x_ref, r_ref,
    marginal_ref, warm_ref, stage, lhi, llo, nhi, nlo, basis, total, vcat, upcat, upper, psend, precv,
    square, table, ridge, mine, others,
    field_sem, load_sem, vs_sem, vr_sem, ps_sem, pr_sem, ms_sem, mr_sem,
):
    me = lax.axis_index("snp")
    traits, block = warm_ref.shape
    count = traits // GROUPS
    tiles = block // TILE
    warm_load = pltpu.make_async_copy(warm_hbm, warm_ref, field_sem.at[0])
    warm_load.start()
    barrier = pltpu.get_barrier_semaphore()
    for k in range(1, n):
        pl.semaphore_signal(barrier, inc=1, device_id={"snp": lax.rem(me + k, n)})

    lane = lax.broadcasted_iota(jnp.int32, (count, 128), 1)
    square[...] = jnp.zeros_like(square)
    square[0:1, :traits] = 1.0 + shrink_ref[...]
    ridge[...] = jnp.transpose(square[...])[:traits]

    def load(i):
        source, width = (next_hbm, (i + 1) * TILE) if i < tiles else (local_hbm, block)
        rows = pl.ds((i % tiles) * TILE, TILE)
        cols = pl.ds(0, width)
        slot = i % slots
        return pltpu.make_async_copy(
            source.at[rows, cols], stage.at[slot, :, cols], load_sem.at[slot]
        )

    for i in range(slots):
        load(i).start()
    marginal_load = pltpu.make_async_copy(marginal_hbm, marginal_ref, field_sem.at[1])
    marginal_load.start()

    def convert(i):
        load(i).wait()
        row = (i % tiles) * TILE
        width = (i + 1) * TILE if i < tiles else block
        for c in range(0, width, TILE):
            piece = stage[i % slots, :, c : c + TILE]
            if i >= tiles and c == row:
                a = lax.broadcasted_iota(jnp.int32, (TILE, TILE), 0)
                b = lax.broadcasted_iota(jnp.int32, (TILE, TILE), 1)
                piece = jnp.where(a == b, 0.0, piece)
            high, low = halves(piece)
            to_high, to_low = (nhi, nlo) if i < tiles else (lhi, llo)
            to_high[row : row + TILE, c : c + TILE] = high
            to_low[row : row + TILE, c : c + TILE] = low
        if i + slots < 2 * tiles:
            load(i + slots).start()

    def group(g):
        return pl.ds(g * count, count)

    def send_field(j, g):
        source = warm_ref.at[group(g)] if j == 0 else basis.at[j - 1, group(g)]
        return pltpu.make_async_remote_copy(
            src_ref=source, dst_ref=upper.at[j, group(g)],
            send_sem=vs_sem.at[j, g], recv_sem=vr_sem.at[j, g],
            device_id={"snp": jnp.maximum(me - 1, 0)},
        )

    def send_coupling(j, g):
        return pltpu.make_async_remote_copy(
            src_ref=psend.at[j, group(g)], dst_ref=precv.at[j, group(g)],
            send_sem=ps_sem.at[j, g], recv_sem=pr_sem.at[j, g],
            device_id={"snp": jnp.minimum(me + 1, n - 1)},
        )

    def times(left, g, high, low, dims, lo_k, hi_k):
        both = lax.dot_general(left[g, :, lo_k:hi_k], high, dims, preferred_element_type=F32)
        rest = lax.dot_general(left[g, :count, lo_k:hi_k], low, dims, preferred_element_type=F32)
        return both[:count] + both[count:] + rest

    def split_into(dest, g, value):
        high, low = halves(value)
        dest[g, :count] = high
        dest[g, count:] = low

    def field(j, g):
        return warm_ref[g * count : (g + 1) * count] if j == 0 else basis[j - 1, g * count : (g + 1) * count]

    def start_field(j, g):
        @pl.when(me > 0)
        def _():
            send_field(j, g).start()

    def coupling(j, g):
        split_into(vcat, g, field(j, g))
        for c in range(0, block, TILE):
            psend[j, g * count : (g + 1) * count, c : c + TILE] = times(
                vcat, g, nhi[c:, c : c + TILE], nlo[c:, c : c + TILE], ROWS, c, block
            )

        @pl.when(me < n - 1)
        def _():
            send_coupling(j, g).start()

    def own(j, g):
        for c in range(0, block, TILE):
            total[g, :, c : c + TILE] = times(
                vcat, g, lhi[:, c : c + TILE], llo[:, c : c + TILE], ROWS, 0, block
            )

    def meet(j, g):
        rows = slice(g * count, (g + 1) * count)

        @pl.when(me < n - 1)
        def _():
            send_field(j, g).wait_recv()

        split_into(upcat, g, upper[j, rows])
        last = jnp.zeros((count, TILE), F32)
        for c in range(0, block, TILE):
            end = c + TILE
            forward = times(upcat, g, nhi[c:end, :end], nlo[c:end, :end], ACROSS, 0, end)
            image = total[g, :, c:end] + forward
            if j == ITERS:
                last += basis[j - 1, rows, c:end] * (image + forward)
            total[g, :, c:end] = image
        if j == ITERS:
            last = jnp.sum(last, axis=1, keepdims=True)
            table[rows] = jnp.where(lane == 2 * ITERS - 1, last, table[rows])

    def finish(j, g):
        rows = slice(g * count, (g + 1) * count)

        @pl.when(me > 0)
        def _():
            send_coupling(j, g).wait_recv()

        image = total[g] + precv[j, rows]
        if j == 0:
            image = marginal_ref[rows] - ridge[rows, :1] * warm_ref[rows] - image
        basis[j, rows] = image

    def moments(g):
        rows = slice(g * count, (g + 1) * count)
        kept = jnp.where(lane == 2 * ITERS, ridge[rows, :1], 0.0)
        for k in range(2 * ITERS - 1):
            sums = jnp.sum(basis[k // 2, rows] * basis[(k + 1) // 2, rows], axis=1, keepdims=True)
            kept = jnp.where(lane == k, sums, kept)
        table[rows] = kept

    @pl.when(me == 0)
    def _():
        precv[...] = jnp.zeros_like(precv)

    @pl.when(me == n - 1)
    def _():
        upper[...] = jnp.zeros_like(upper)

    warm_load.wait()
    pl.semaphore_wait(barrier, n - 1)
    for g in range(GROUPS):
        start_field(0, g)
    for i in range(tiles):
        convert(i)
    for g in range(GROUPS):
        coupling(0, g)
    for i in range(tiles, 2 * tiles):
        convert(i)
    for g in range(GROUPS):
        own(0, g)
    marginal_load.wait()
    for j in range(ITERS):
        for g in range(GROUPS):
            meet(j, g)
            finish(j, g)
            start_field(j + 1, g)
            coupling(j + 1, g)
            own(j + 1, g)
            if j + 1 == ITERS:
                moments(g)
    for g in range(GROUPS):
        meet(ITERS, g)

    square[:traits] = table[...]
    flat = jnp.transpose(square[...])
    mine[...] = flat[:8]
    others[me] = flat[:8]

    def send_sums(k):
        return pltpu.make_async_remote_copy(
            src_ref=mine, dst_ref=others.at[me],
            send_sem=ms_sem.at[k], recv_sem=mr_sem.at[me],
            device_id={"snp": lax.rem(me + k, n)},
        )

    def take_sums(k):
        source = lax.rem(me + k, n)
        return pltpu.make_async_remote_copy(
            src_ref=mine, dst_ref=others.at[source],
            send_sem=ms_sem.at[k], recv_sem=mr_sem.at[source],
            device_id={"snp": source},
        )

    for k in range(1, n):
        send_sums(k).start()
    for k in range(1, n):
        take_sums(k).wait_recv()
    sums = others[0]
    for k in range(1, n):
        sums = sums + others[k]
    moment = [sums[k : k + 1] for k in range(2 * ITERS)]
    update, residual = scalars(moment, mine[2 * ITERS : 2 * ITERS + 1])
    for k, row in enumerate(update + residual):
        square[k : k + 1] = row
    tall = jnp.transpose(square[...])[:traits]
    x = warm_ref[...]
    for k in range(ITERS):
        x = x + tall[:, k : k + 1] * basis[k]
    x_ref[...] = x
    for g in range(GROUPS):
        rows = slice(g * count, (g + 1) * count)
        r = tall[rows, 2 * ITERS : 2 * ITERS + 1] * total[g]
        for k in range(ITERS):
            r = r + tall[rows, ITERS + k : ITERS + k + 1] * basis[k, rows]
        r_ref[rows] = r
    for g in range(GROUPS):
        rows = slice(g * count, (g + 1) * count)

        @pl.when(me > 0)
        def _():
            send_coupling(ITERS, g).wait_recv()

        r_ref[rows] += tall[rows, 2 * ITERS : 2 * ITERS + 1] * precv[ITERS, rows]

    for k in range(1, n):
        send_sums(k).wait_send()

    @pl.when(me > 0)
    def _():
        for j in range(ITERS + 1):
            for g in range(GROUPS):
                send_field(j, g).wait_send()

    @pl.when(me < n - 1)
    def _():
        for j in range(ITERS + 1):
            for g in range(GROUPS):
                send_coupling(j, g).wait_send()


def hand_on(x_in, r_in, x_ref, r_ref):
    x_ref[...] = x_in[...]
    r_ref[...] = r_in[...]


def on_device(local_block, next_block, shrinkage, marginal, warm_start):
    n = lax.axis_size("snp")
    traits, block = warm_start.shape
    count = traits // GROUPS
    slots = min(2 * (block // TILE), 8 if block <= 1024 else 4)
    apps = ITERS + 1
    vmem = pl.BlockSpec(memory_space=pltpu.VMEM)
    hbm = pl.BlockSpec(memory_space=pltpu.HBM)
    field = (apps, traits, block)
    x, r = pl.pallas_call(
        functools.partial(kernel, n, slots),
        name="cg",
        out_shape=[jax.ShapeDtypeStruct((traits, block), F32)] * 2,
        in_specs=[hbm, hbm, vmem, hbm, hbm],
        out_specs=[vmem] * 2,
        scratch_shapes=[
            pltpu.VMEM((traits, block), F32),
            pltpu.VMEM((traits, block), F32),
            pltpu.VMEM((slots, TILE, block), F32),
            pltpu.VMEM((block, block), BF16),
            pltpu.VMEM((block, block), BF16),
            pltpu.VMEM((block, block), BF16),
            pltpu.VMEM((block, block), BF16),
            pltpu.VMEM((ITERS, traits, block), F32),
            pltpu.VMEM((GROUPS, count, block), F32),
            pltpu.VMEM((GROUPS, 2 * count, block), BF16),
            pltpu.VMEM((GROUPS, 2 * count, block), BF16),
            pltpu.VMEM(field, F32),
            pltpu.VMEM(field, F32),
            pltpu.VMEM(field, F32),
            pltpu.VMEM((128, 128), F32),
            pltpu.VMEM((traits, 128), F32),
            pltpu.VMEM((traits, 128), F32),
            pltpu.VMEM((8, 128), F32),
            pltpu.VMEM((n, 8, 128), F32),
            pltpu.SemaphoreType.DMA((2,)),
            pltpu.SemaphoreType.DMA((slots,)),
            pltpu.SemaphoreType.DMA((apps, GROUPS)),
            pltpu.SemaphoreType.DMA((apps, GROUPS)),
            pltpu.SemaphoreType.DMA((apps, GROUPS)),
            pltpu.SemaphoreType.DMA((apps, GROUPS)),
            pltpu.SemaphoreType.DMA((n,)),
            pltpu.SemaphoreType.DMA((n,)),
        ],
        compiler_params=pltpu.CompilerParams(
            collective_id=0, has_side_effects=True, vmem_limit_bytes=61 << 20
        ),
    )(local_block, next_block, shrinkage.reshape(1, traits), marginal, warm_start)
    return pl.pallas_call(
        hand_on,
        name="hand_on",
        out_shape=[jax.ShapeDtypeStruct((traits, block), F32)] * 2,
        in_specs=[vmem] * 2,
        out_specs=[vmem] * 2,
    )(x, r)


def solution(mesh):
    return jax.shard_map(
        on_device,
        mesh=mesh,
        in_specs=(
            P(("parts", "snp"), None),
            P(("parts", "snp"), None),
            P(),
            P(None, ("parts", "snp")),
            P(None, ("parts", "snp")),
        ),
        out_specs=(P(None, ("parts", "snp")), P(None, ("parts", "snp"))),
        check_vma=False,
    )
```
